32 devices in a mesh: wide: 8 (over z, y), narrow: 4 (over x, core).
Axes of the slice: x: 2, y: 2, z: 4, core: 2. Of those that a mesh axis runs over, the one named last changes fastest.
Arguments:
- hidden: bfloat16 [64, 16384], P('narrow', 'wide'), may hold values from -6 to 6
- gain: bfloat16 [16384], P('wide'), may hold values from 0.5 to 1.5
- sign_in: int32 [16384], P('wide'), may hold values from 0 to 1
- qkv_weight: bfloat16 [16384, 18432], P('wide', 'narrow'), may hold values from -0.046875 to 0.046875
- out_weight: bfloat16 [16384, 16384], P('narrow', 'wide'), may hold values from -0.046875 to 0.046875
- sign_attn: int32 [16384], P('narrow'), may hold values from 0 to 1
- key_cache: bfloat16 [64, 8, 4096, 128], P('wide', 'narrow'), may hold values from -512 to 512, as said below
- value_cache: bfloat16 [64, 8, 4096, 128], P('wide', 'narrow'), may hold values from -6 to 6
- lengths: int32 [64], P('wide'), may hold values from 1024 to 4096
Outputs:
- layer_out: bfloat16 [64, 16384], P('narrow', 'wide')
The draws below stay inside these ranges and needn't reach their ends.
Inputs may be any that keep to these rules, and one draw needn't show every extreme that they name: `key_cache`: cached keys mostly of magnitude about 2, with some slots far larger in the hidden draw.
All inputs are finite; a program needn't handle non-finite values. Where the reference program divides by a largest or mean magnitude, that divisor is 1e-20 or more.
Results may differ from the reference program's by a relative error of at most 0.018.
Values may be sent and summed in bfloat16 or wider, within the bound.
A program may use at most 128 MiB of HBM per device.

```python
import math
import jax
import jax.numpy as jnp
from jax import lax

D = 16384
HQ = 128
KVH = 8
HD = 128
S = 4096
LISTS = 64
QG = 16


def draw_key_cache(key, part):
    normal_keys = jax.random.normal(jax.random.fold_in(key, 11), (LISTS, KVH, S, HD), jnp.float32) * 2.0
    normal_keys = jnp.clip(normal_keys, -12.0, 12.0)
    return normal_keys.astype(jnp.bfloat16)


def touch_ends(result, own_key, least, largest):
    extent = result.shape
    index_at = [jax.random.randint(jax.random.fold_in(own_key, axis), (), 0, extent[axis]) for axis in range(len(extent))]
    result = result.at[tuple(index_at)].set(least)
    longest = extent.index(max(extent))
    index_at[longest] = (index_at[longest] + 1) % extent[longest]
    return result.at[tuple(index_at)].set(largest)


def shard_levels(rng, extent, cuts, smallest, top_value):
    level, own = 1.0, jax.random.fold_in(rng, 6)
    for position, shards_of in cuts:
        heights = jnp.exp(jax.random.uniform(jax.random.fold_in(own, position), (shards_of,), jnp.float32, smallest / len(cuts), top_value / len(cuts)))
        level = level * jnp.repeat(heights, extent[position] // shards_of).reshape([-1 if axis == position else 1 for axis in range(len(extent))])
    return level


def bell_draw(rng, shape, deviation, reach, cuts=(), kind=jnp.bfloat16):
    level = shard_levels(rng, shape, cuts, -0.22, 0.18) if cuts else 1.0
    entries = jax.random.normal(rng, shape, jnp.float32) * deviation * level
    return jnp.minimum(jnp.maximum(entries, -reach), reach).astype(kind)


def setup_inputs(seed: int = 0) -> dict:
    key_list = jax.random.split(jax.random.key(seed), 10)
    hidden = bell_draw(key_list[0], (LISTS, D), 1.0, 6.0, ((0, 4), (1, 8)))
    gain = jnp.clip(1.0 + 0.1 * jax.random.normal(key_list[1], (D,), jnp.float32), 0.5, 1.5).astype(jnp.bfloat16)
    sign_in = touch_ends(jax.random.randint(key_list[2], (D,), 0, 2), jax.random.fold_in(key_list[2], 1), 0, 1).astype(jnp.int32)
    qkv_weight = bell_draw(key_list[3], (D, KVH * (QG + 2) * HD), D ** -0.5, 0.046875, ((0, 8), (1, 4)))
    out_weight = bell_draw(key_list[4], (HQ * HD, D), (HQ * HD) ** -0.5, 0.046875, ((0, 4), (1, 8)))
    sign_attn = touch_ends(jax.random.randint(key_list[5], (HQ * HD,), 0, 2), jax.random.fold_in(key_list[5], 1), 0, 1).astype(jnp.int32)
    key_cache = draw_key_cache(jax.random.fold_in(key_list[9], 71), 0)
    value_cache = bell_draw(key_list[7], (LISTS, KVH, S, HD), 1.0, 6.0, ((0, 8), (1, 4)))
    lengths = touch_ends(jax.random.randint(key_list[8], (LISTS,), S // 4, S + 1), jax.random.fold_in(key_list[8], 1), S // 4, S).astype(jnp.int32)
    return {"hidden": hidden, "gain": gain, "sign_in": sign_in, "qkv_weight": qkv_weight, "out_weight": out_weight, "sign_attn": sign_attn, "key_cache": key_cache, "value_cache": value_cache, "lengths": lengths}


ROPE_BASE = 500000.0

def hadamard(order):
    places = jnp.arange(order, dtype=jnp.int32)
    common = places[:, None] & places[None, :]
    parity = jnp.zeros((order, order), jnp.int32)
    for bit_pos in range(order.bit_length() - 1):
        parity = parity ^ common >> bit_pos & 1
    return (1 - 2 * parity).astype(jnp.float32) / math.sqrt(order)

def rotate_blocks(values, sign_bits, width):
    signs = (2 * sign_bits - 1).astype(jnp.float32)
    blocks = (values * signs).reshape(values.shape[:-1] + (values.shape[-1] // width, width))
    turned = jnp.einsum('...bk,kj->...bj', blocks, hadamard(width), precision=lax.Precision.HIGHEST)
    scales = (lax.optimization_barrier(jnp.max(jnp.abs(turned), axis=-1)) + 1e-06).astype(jnp.bfloat16)
    payload = (turned / scales.astype(jnp.float32)[..., None]).astype(jnp.bfloat16)
    return (payload, scales)

def rotary(vectors, positions):
    half_width = vectors.shape[-1] // 2
    frequency = jnp.exp(jnp.arange(half_width, dtype=jnp.float32) * (-2.0 * math.log(ROPE_BASE) / vectors.shape[-1]))
    angles = positions.astype(jnp.float32)[:, None] * frequency[None, :]
    cosine = jnp.cos(angles)[:, None, :]
    sines = jnp.sin(angles)[:, None, :]
    lower_half = vectors[..., :half_width]
    upper_half = vectors[..., half_width:]
    return jnp.concatenate([lower_half * cosine - upper_half * sines, upper_half * cosine + lower_half * sines], axis=-1)

def reference(hidden, gain, sign_in, qkv_weight, out_weight, sign_attn, key_cache, value_cache, lengths):
    rows = hidden.astype(jnp.float32)
    factor = lax.rsqrt(lax.optimization_barrier(jnp.sum(rows * rows, axis=1)) / D + 1e-05)
    normed = rows * factor[:, None] * gain.astype(jnp.float32)[None, :]
    payload, scales = rotate_blocks(normed, sign_in, HD)
    weight_blocks = qkv_weight.reshape(D // HD, HD, qkv_weight.shape[1])

    def add_block(total, inputs):
        block_rows, block_scale, block_weight = inputs
        product = jnp.dot(block_rows, block_weight, preferred_element_type=jnp.float32)
        return (total + block_scale.astype(jnp.float32)[:, None] * product, None)
    start_total = jnp.zeros((LISTS, qkv_weight.shape[1]), jnp.float32)
    projected, _ = lax.scan(add_block, start_total, (jnp.swapaxes(payload, 0, 1), jnp.swapaxes(scales, 0, 1), weight_blocks))
    grouped = projected.reshape(LISTS, KVH, QG + 2, HD)
    queries = rotary(grouped[:, :, :QG, :].reshape(LISTS, KVH * QG, HD), lengths)
    queries = queries.astype(jnp.bfloat16).reshape(LISTS, KVH, QG, HD)
    keys_new = rotary(grouped[:, :, QG, :], lengths).astype(jnp.bfloat16)
    values_new = grouped[:, :, QG + 1, :].astype(jnp.bfloat16)
    inverse_root = 1.0 / math.sqrt(HD)

    def attend(inputs):
        query, key_new, value_new, keys, values, length = inputs
        query_f = query.astype(jnp.float32)
        scores = jnp.einsum('gqk,gsk->gqs', query_f, keys.astype(jnp.float32)) * inverse_root
        fresh = jnp.einsum('gqk,gk->gq', query_f, key_new.astype(jnp.float32)) * inverse_root
        live = jnp.arange(S, dtype=jnp.int32) < length
        scores = jnp.where(live[None, None, :], scores, -1e+30)
        peak = jnp.maximum(lax.optimization_barrier(jnp.max(scores, axis=-1)), fresh)
        weights = jnp.where(live[None, None, :], jnp.exp(scores - peak[..., None]), 0.0)
        weight_new = jnp.exp(fresh - peak)
        denom_sum = lax.optimization_barrier(jnp.sum(weights, axis=-1)) + weight_new
        probs = (weights / denom_sum[..., None]).astype(jnp.bfloat16)
        prob_new = (weight_new / denom_sum).astype(jnp.bfloat16)
        mixed = jnp.einsum('gqs,gsk->gqk', probs.astype(jnp.float32), values.astype(jnp.float32))
        return mixed + prob_new.astype(jnp.float32)[..., None] * value_new.astype(jnp.float32)[:, None, :]
    attended = lax.map(attend, (queries, keys_new, values_new, key_cache, value_cache, lengths))
    out_blocks, out_scale = rotate_blocks(attended.reshape(LISTS, HQ * HD), sign_attn, HD)
    head_weights = out_weight.reshape(HQ, HD, D)

    def add_head(total, inputs):
        head_rows, head_scale, head_weight = inputs
        product = jnp.dot(head_rows, head_weight, preferred_element_type=jnp.float32)
        return (total + head_scale.astype(jnp.float32)[:, None] * product, None)
    mixed, _ = lax.scan(add_head, jnp.zeros((LISTS, D), jnp.float32), (jnp.swapaxes(out_blocks, 0, 1), jnp.swapaxes(out_scale, 0, 1), head_weights))
    return (rows + mixed).astype(jnp.bfloat16)
```

```python
import math

import jax
import jax.numpy as jnp
from jax import lax
from jax.experimental import pallas as pl
from jax.experimental.pallas import tpu as pltpu
from jax.sharding import PartitionSpec as P

MESH = pl.DeviceIdType.MESH

D = 16384
HD = 128
QG = 16


ROPE_BASE = 500000.0


def hadamard(order):
    places = jnp.arange(order, dtype=jnp.int32)
    common = places[:, None] & places[None, :]
    parity = jnp.zeros((order, order), jnp.int32)
    for bit_pos in range(order.bit_length() - 1):
        parity = parity ^ common >> bit_pos & 1
    return (1 - 2 * parity).astype(jnp.float32) / math.sqrt(order)


def rotate_blocks(values, sign_bits, width):
    signs = (2 * sign_bits - 1).astype(jnp.float32)
    blocks = (values * signs).reshape(values.shape[:-1] + (values.shape[-1] // width, width))
    turned = jnp.einsum("...bk,kj->...bj", blocks, hadamard(width), precision=lax.Precision.HIGHEST)
    scales = (jnp.max(jnp.abs(turned), axis=-1) + 1e-06).astype(jnp.bfloat16)
    payload = turned / scales.astype(jnp.float32)[..., None]
    return (payload, scales)


def rotary(vectors, positions):
    half_width = vectors.shape[-1] // 2
    frequency = jnp.exp(
        jnp.arange(half_width, dtype=jnp.float32) * (-2.0 * math.log(ROPE_BASE) / vectors.shape[-1])
    )
    angles = positions.astype(jnp.float32)[:, None] * frequency[None, :]
    cosine = jnp.cos(angles)[:, None, :]
    sines = jnp.sin(angles)[:, None, :]
    lower_half = vectors[..., :half_width]
    upper_half = vectors[..., half_width:]
    return jnp.concatenate(
        [lower_half * cosine - upper_half * sines, upper_half * cosine + lower_half * sines],
        axis=-1,
    )


def exchange(x, axis, cid, gather, reduce):
    n = lax.axis_size(axis)
    part = x.shape if gather else x.shape[1:]

    def kernel(x_ref, o_ref, held, send_sem, recv_sem, own_sem):
        me = lax.axis_index(axis)
        barrier = pltpu.get_barrier_semaphore()
        for k in range(1, n):
            pl.semaphore_signal(
                barrier, inc=1, device_id={axis: lax.rem(me + k, n)}, device_id_type=MESH
            )
        pl.semaphore_wait(barrier, n - 1)
        copies = []
        for k in range(1, n):
            peer = lax.rem(me + k, n)
            copies.append(
                pltpu.make_async_remote_copy(
                    src_ref=x_ref if gather else x_ref.at[peer],
                    dst_ref=held.at[me],
                    send_sem=send_sem.at[k],
                    recv_sem=recv_sem.at[k],
                    device_id={axis: peer},
                    device_id_type=MESH,
                )
            )
            copies[-1].start()
        own = pltpu.make_async_copy(x_ref if gather else x_ref.at[me], held.at[me], own_sem)
        own.start()
        own.wait()
        for copy in copies:
            copy.wait()
        if reduce:
            total = held[0].astype(jnp.float32)
            for k in range(1, n):
                total = total + held[k].astype(jnp.float32)
            o_ref[...] = total
        else:
            o_ref[...] = held[...]

    out = (
        jax.ShapeDtypeStruct(part, jnp.float32)
        if reduce
        else jax.ShapeDtypeStruct((n,) + part, x.dtype)
    )
    return pl.pallas_call(
        kernel,
        out_shape=out,
        in_specs=[pl.BlockSpec(memory_space=pltpu.VMEM)],
        out_specs=pl.BlockSpec(memory_space=pltpu.VMEM),
        scratch_shapes=[
            pltpu.VMEM((n,) + part, x.dtype),
            pltpu.SemaphoreType.DMA((n,)),
            pltpu.SemaphoreType.DMA((n,)),
            pltpu.SemaphoreType.DMA,
        ],
        compiler_params=pltpu.CompilerParams(
            collective_id=cid, has_side_effects=True, vmem_limit_bytes=24 * 2**20
        ),
        name=f"exchange{cid}",
    )(x)


def attention(queries, keys_new, values_new, key_cache, value_cache, lengths):
    lists, groups, slots, hd = key_cache.shape
    chunk = 1024 if slots % 1024 == 0 else slots
    steps = slots // chunk
    inverse_root = 1.0 / math.sqrt(HD)

    def kernel(len_ref, q_ref, kn_ref, vn_ref, k_ref, v_ref, o_ref, top, den, acc):
        i, c = pl.program_id(0), pl.program_id(1)
        length = len_ref[i]

        @pl.when(c == 0)
        def _():
            for g in range(groups):
                q = q_ref[0, g].astype(jnp.float32)
                fresh = jnp.sum(q * kn_ref[0, g], axis=-1, keepdims=True) * inverse_root
                top[g] = jnp.broadcast_to(fresh, (QG, hd))
                den[g] = jnp.ones((QG, hd), jnp.float32)
                acc[g] = jnp.broadcast_to(vn_ref[0, g], (QG, hd))

        @pl.when(c * chunk < length)
        def _():
            place = c * chunk + lax.broadcasted_iota(jnp.int32, (QG, chunk), 1)
            live = place < length
            for g in range(groups):
                scores = (
                    lax.dot_general(
                        q_ref[0, g],
                        k_ref[0, g],
                        (((1,), (1,)), ((), ())),
                        preferred_element_type=jnp.float32,
                    )
                    * inverse_root
                )
                scores = jnp.where(live, scores, -1e30)
                before = top[g][:, :1]
                peak = jnp.maximum(before, jnp.max(scores, axis=-1, keepdims=True))
                weights = jnp.where(live, jnp.exp(scores - peak), 0.0)
                shrink = jnp.exp(before - peak)
                top[g] = jnp.broadcast_to(peak, (QG, hd))
                den[g] = den[g] * shrink + jnp.sum(weights, axis=-1, keepdims=True)
                acc[g] = acc[g] * shrink + jnp.dot(
                    weights.astype(jnp.bfloat16), v_ref[0, g], preferred_element_type=jnp.float32
                )

        @pl.when(c == steps - 1)
        def _():
            for g in range(groups):
                o_ref[0, g] = acc[g] / den[g]

    def cache_map(i, c, len_ref):
        last = (len_ref[i] + chunk - 1) // chunk - 1
        return (i, 0, jnp.minimum(c, last), 0)

    def small(rows):
        return pl.BlockSpec((1, groups, rows, hd), lambda i, c, len_ref: (i, 0, 0, 0))

    return pl.pallas_call(
        kernel,
        grid_spec=pltpu.PrefetchScalarGridSpec(
            num_scalar_prefetch=1,
            grid=(lists, steps),
            in_specs=[
                small(QG),
                small(1),
                small(1),
                pl.BlockSpec((1, groups, chunk, hd), cache_map),
                pl.BlockSpec((1, groups, chunk, hd), cache_map),
            ],
            out_specs=small(QG),
            scratch_shapes=[pltpu.VMEM((groups, QG, hd), jnp.float32)] * 3,
        ),
        out_shape=jax.ShapeDtypeStruct((lists, groups, QG, hd), jnp.float32),
        compiler_params=pltpu.CompilerParams(vmem_limit_bytes=32 * 2**20),
        name="attention",
    )(lengths, queries, keys_new, values_new, key_cache, value_cache)


def scaled(payload, scales, shape):
    return (payload * scales.astype(jnp.float32)[..., None]).astype(jnp.bfloat16).reshape(shape)


def body(hidden, gain, sign_in, qkv_weight, out_weight, sign_attn, key_cache, value_cache, lengths):
    rows = hidden.astype(jnp.float32)
    squares = jnp.broadcast_to(jnp.sum(rows * rows, axis=1, keepdims=True), (rows.shape[0], HD))
    squares = exchange(squares, "wide", 1, True, True)[:, :1]
    factor = lax.rsqrt(squares / D + 1e-05)
    normed = rows * factor * gain.astype(jnp.float32)[None, :]
    payload, scales = rotate_blocks(normed, sign_in, HD)
    own = scaled(payload, scales, hidden.shape)
    every = exchange(own, "narrow", 2, True, False).reshape(-1, hidden.shape[1])
    lists, groups = key_cache.shape[:2]
    partial = jnp.dot(every, qkv_weight, preferred_element_type=jnp.float32).astype(jnp.bfloat16)
    projected = exchange(partial.reshape(-1, lists, partial.shape[1]), "wide", 3, False, True)
    grouped = projected.reshape(lists, groups, QG + 2, HD)
    turned = rotary(grouped[:, :, : QG + 1, :].reshape(lists, groups * (QG + 1), HD), lengths)
    turned = turned.astype(jnp.bfloat16).reshape(lists, groups, QG + 1, HD)
    values_new = grouped[:, :, QG + 1 :, :].astype(jnp.bfloat16).astype(jnp.float32)
    attended = attention(
        turned[:, :, :QG],
        turned[:, :, QG:].astype(jnp.float32),
        values_new,
        key_cache,
        value_cache,
        lengths,
    )
    width = groups * QG * HD
    payload, scales = rotate_blocks(attended.reshape(lists, width), sign_attn, HD)
    heads = exchange(scaled(payload, scales, (lists, width)), "wide", 4, True, False)
    mixed = jnp.dot(
        heads.reshape(-1, width), out_weight, preferred_element_type=jnp.float32
    ).astype(jnp.bfloat16)
    mixed = exchange(mixed.reshape(-1, hidden.shape[0], mixed.shape[1]), "narrow", 5, False, True)
    return (rows + mixed).astype(jnp.bfloat16)


def solution(mesh):
    in_specs = (
        P("narrow", "wide"),
        P("wide"),
        P("wide"),
        P("wide", "narrow"),
        P("narrow", "wide"),
        P("narrow"),
        P("wide", "narrow", None, None),
        P("wide", "narrow", None, None),
        P("wide"),
    )
    out_specs = P("narrow", "wide")
    return jax.shard_map(body, mesh=mesh, in_specs=in_specs, out_specs=out_specs, check_vma=False)
```
